32 devices in a mesh: dp: 4 (over y, x), group: 8 (over z, core).
Axes of the slice: x: 2, y: 2, z: 4, core: 2. Of those that a mesh axis runs over, the one named last changes fastest.
Arguments:
- tokens: bfloat16 [2048, 5120], P('dp'), may hold values from -6 to 6
- frame_mask: int32 [2048], P('dp'), may hold values 0 or 1
- cotangent: bfloat16 [2048, 5120], P('dp'), may hold values from -0.625 to 0.625
- up_weight: bfloat16 [5120, 8192], P('dp', 'group'), may hold values from -0.078125 to 0.078125
- down_weight: bfloat16 [5120, 8192], P('dp', 'group'), may hold values from -0.0625 to 0.0625
- snap_params: bfloat16 [8, 32768], P(None, ('dp', 'group')), may hold values from -6 to 6
- first_moment: float32 [8, 32768], P(None, ('dp', 'group')), may hold values from -6 to 6
- second_moment: float32 [8, 32768], P(None, ('dp', 'group')), may hold values from 0.01 to 4
- range_of_writer: int32 [8], replicated, may hold values from 0 to 7, each once
Outputs:
- grad_up: float32 [5120, 8192], P('dp', 'group')
- grad_down: float32 [5120, 8192], P('dp', 'group')
- written_params: bfloat16 [8, 32768], P('group', 'dp')
- written_moments: float32 [2, 8, 32768], P(None, 'group', 'dp')
The draws below stay inside these ranges and needn't reach their ends.
Inputs may be any that keep to these rules, and one draw needn't show every extreme that they name: `range_of_writer`: each of the 8 ranges is named by exactly one owner.
All inputs are finite; a program needn't handle non-finite values. No bound on the sum of `frame_mask` on one device may be relied on, other than what follows from the above.
Results may differ from the reference program's by a relative error of at most 0.017.
Values may be sent and summed in bfloat16 or wider, within the bound.
A program may use at most 128 MiB of HBM per device.

```python
import math
import jax
import jax.numpy as jnp
from jax import lax

D = 5120
FF = 8192
TOK_DEV = 512
TOKENS = 2048
RANGES = 8
FLAT = 32768
N_DP = 4
N_GROUP = 8


def set_ends(values, own_key, low, top_value):
    spot = [jax.random.randint(jax.random.fold_in(own_key, axis), (), 0, length) for axis, length in enumerate(values.shape)]
    widest = values.shape.index(max(values.shape))
    beside = spot[:widest] + [(spot[widest] + 1) % values.shape[widest]] + spot[widest + 1:]
    return values.at[tuple(spot)].set(low).at[tuple(beside)].set(top_value)


def raised(entries, key, source, target, blocks, factor):
    owner, partner = [(jnp.arange(entries.shape[axis_at]) // (entries.shape[axis_at] // blocks)).reshape([-1 if axis == axis_at else 1 for axis in range(entries.ndim)]) for axis_at in (source, target)]
    chosen = jax.random.permutation(key, blocks)[partner]
    strong = (owner == chosen) | (owner == (partner + blocks // 2) % blocks)
    return jnp.where(strong, factor * entries, entries)


def levels(rng, shape, cuts, smallest, largest):
    loudness = 1.0
    for dim, shards_of in cuts:
        heights = jax.random.uniform(jax.random.fold_in(jax.random.fold_in(rng, 6), dim), (shards_of,), jnp.float32, smallest / len(cuts), largest / len(cuts))
        loudness = loudness * jnp.repeat(jnp.exp(heights), shape[dim] // shards_of).reshape((-1,) + (1,) * (len(shape) - 1 - dim))
    return loudness


def bell_draw(key, dims, deviation, most, cuts=(), held_as=jnp.bfloat16):
    level = levels(key, dims, cuts, -0.22, 0.18) if cuts else 1.0
    drawn = jax.random.normal(key, dims, jnp.float32) * deviation * level
    return jnp.minimum(jnp.maximum(drawn, -most), most).astype(held_as)


def bell_draw_with(own_key, shape, deviation, reach, split, heavy, kind=jnp.bfloat16):
    array = deviation * jax.random.normal(own_key, shape, jnp.float32)
    if split:
        array = array * levels(own_key, shape, split, -0.22, 0.18)
    return jnp.clip(raised(array, jax.random.fold_in(own_key, 3), *heavy), -reach, reach).astype(kind)


def setup_inputs(seed: int = 0) -> dict:
    seeds = jax.random.split(jax.random.key(seed), 10)
    return {
        "tokens": bell_draw(seeds[0], (TOKENS, D), 1.0, 6.0, ((0, 4),)),
        "frame_mask": set_ends((jax.random.randint(seeds[1], (TOKENS,), 0, 4) < 3).astype(jnp.int32), jax.random.fold_in(seeds[1], 1), 0, 1),
        "cotangent": bell_draw_with(seeds[2], (TOKENS, D), 0.03, 0.625, ((0, 4),), (0, 1, 4, 2.0)),
        "up_weight": bell_draw(seeds[3], (D, FF), D ** -0.5, 0.078125, ((0, 4), (1, 8))),
        "down_weight": bell_draw(seeds[4], (D, FF), FF ** -0.5, 0.0625, ((0, 4), (1, 8))),
        "snap_params": bell_draw(seeds[5], (RANGES, FLAT), 0.5, 6.0, ((1, 32),)),
        "first_moment": bell_draw(seeds[6], (RANGES, FLAT), 0.5, 6.0, ((1, 32),), jnp.float32),
        "second_moment": jnp.clip(jnp.exp(math.log(4.0) - 5.9914646 * jax.random.uniform(seeds[7], (RANGES, FLAT), jnp.float32) ** levels(seeds[7], (RANGES, FLAT), ((1, 32),), -0.2, 0.2)), 0.01, 4.0),
        "range_of_writer": jax.random.permutation(seeds[8], N_GROUP).astype(jnp.int32),
    }


EPS = 1e-06

def normalize(tokens):
    values = tokens.astype(jnp.float32)
    centred = values - lax.optimization_barrier(jnp.mean(values, axis=1, keepdims=True))
    spread = lax.optimization_barrier(jnp.mean(centred * centred, axis=1, keepdims=True))
    return (centred * lax.rsqrt(spread + EPS)).astype(jnp.bfloat16)

def gelu_pair(pre, d_act):
    act, pullback = jax.vjp(lambda v: jax.nn.gelu(v, approximate=True), pre)
    return (act.astype(jnp.bfloat16), pullback(d_act)[0].astype(jnp.bfloat16))

def outer_sum(left, right):
    return lax.dot_general(left, right, (((0,), (0,)), ((), ())), preferred_element_type=jnp.float32)

def reference(tokens, frame_mask, cotangent, up_weight, down_weight, snap_params, first_moment, second_moment, range_of_writer):
    normed = normalize(tokens)
    masked = cotangent * frame_mask[:, None].astype(jnp.bfloat16)
    pre = jnp.dot(normed, up_weight, preferred_element_type=jnp.float32)
    d_act = jnp.dot(masked, down_weight, preferred_element_type=jnp.float32)
    act, grad_pre = gelu_pair(pre, d_act)
    blocks = (normed.reshape(N_DP, TOK_DEV, D), grad_pre.reshape(N_DP, TOK_DEV, FF), masked.reshape(N_DP, TOK_DEV, D), act.reshape(N_DP, TOK_DEV, FF))

    def accumulate(totals, block):
        n_blk, g_blk, m_blk, a_blk = block
        up_part = lax.optimization_barrier(outer_sum(n_blk, g_blk).astype(jnp.bfloat16)).astype(jnp.float32)
        down_part = lax.optimization_barrier(outer_sum(m_blk, a_blk).astype(jnp.bfloat16)).astype(jnp.float32)
        return ((totals[0] + up_part, totals[1] + down_part), None)
    empty = jnp.zeros((D, FF), jnp.float32)
    (grad_up, grad_down), _ = lax.scan(accumulate, (empty, empty), blocks)
    order = range_of_writer.astype(jnp.int32)
    written_params = snap_params[order]
    written_moments = jnp.stack([first_moment[order], second_moment[order]])
    return (grad_up, grad_down, written_params, written_moments)
```

```python
import jax
import jax.numpy as jnp
from jax import lax
from jax.sharding import PartitionSpec as P

EPS = 1e-06


def normalize(tokens):
    values = tokens.astype(jnp.float32)
    centred = values - jnp.mean(values, axis=1, keepdims=True)
    spread = jnp.mean(centred * centred, axis=1, keepdims=True)
    return (centred * lax.rsqrt(spread + EPS)).astype(jnp.bfloat16)


def gelu_pair(pre, d_act):
    act, pullback = jax.vjp(lambda v: jax.nn.gelu(v, approximate=True), pre)
    return (act.astype(jnp.bfloat16), pullback(d_act)[0].astype(jnp.bfloat16))


def outer_sum(left, right):
    return lax.dot_general(
        left, right, (((0,), (0,)), ((), ())), preferred_element_type=jnp.float32
    )


def regroup(snap_params, first_moment, second_moment, range_of_writer):
    flat = snap_params.shape[1]
    held = jnp.concatenate(
        [snap_params, first_moment.astype(jnp.bfloat16), second_moment.astype(jnp.bfloat16)],
        axis=1,
    )
    send = jnp.take(held, range_of_writer, axis=0).reshape(-1, 3, flat)
    got = lax.all_to_all(send, "group", split_axis=0, concat_axis=0, tiled=True)
    lines = jnp.swapaxes(got, 0, 1).reshape(3, 1, -1)
    return lines[0], lines[1:].astype(first_moment.dtype)


def per_device(
    tokens,
    frame_mask,
    cotangent,
    up_weight,
    down_weight,
    snap_params,
    first_moment,
    second_moment,
    range_of_writer,
):
    written = regroup(snap_params, first_moment, second_moment, range_of_writer)
    rows = tokens.shape[0] // lax.axis_size("group")
    first = lax.axis_index("group") * rows
    own_tokens = lax.dynamic_slice_in_dim(tokens, first, rows, axis=0)
    own_mask = lax.dynamic_slice_in_dim(frame_mask, first, rows, axis=0)
    own_cotangent = lax.dynamic_slice_in_dim(cotangent, first, rows, axis=0)
    normed = normalize(own_tokens)
    masked = own_cotangent * own_mask[:, None].astype(jnp.bfloat16)

    def to_features(rows_here):
        part = lax.all_to_all(rows_here, "dp", split_axis=1, concat_axis=0, tiled=True)
        return lax.all_gather(part, "group", axis=0, tiled=True)

    def own_rows_total(left, weight):
        part = jnp.dot(left, weight, preferred_element_type=jnp.float32).astype(jnp.bfloat16)
        return lax.psum_scatter(part, "dp", scatter_dimension=0, tiled=True)

    normed = to_features(normed)
    masked = to_features(masked)
    pre = own_rows_total(normed, up_weight)
    d_act = own_rows_total(masked, down_weight)
    act, grad_pre = gelu_pair(pre.astype(jnp.float32), d_act.astype(jnp.float32))
    grad_down = outer_sum(masked, lax.all_gather(act, "dp", axis=0, tiled=True))
    grad_up = outer_sum(normed, lax.all_gather(grad_pre, "dp", axis=0, tiled=True))
    return (grad_up, grad_down, written[0], written[1])


def solution(mesh):
    placed = (
        P("dp", None),
        P("dp"),
        P("dp", None),
        P("dp", "group"),
        P("dp", "group"),
        P(None, ("dp", "group")),
        P(None, ("dp", "group")),
        P(None, ("dp", "group")),
        P(),
    )
    return jax.shard_map(
        per_device,
        mesh=mesh,
        in_specs=placed,
        out_specs=(P("dp", "group"), P("dp", "group"), P("group", "dp"), P(None, "group", "dp")),
        check_vma=False,
    )
```

```python
import jax
import jax.numpy as jnp
from jax import lax
from jax.sharding import PartitionSpec as P

EPS = 1e-06


def normalize(tokens):
    values = tokens.astype(jnp.float32)
    centred = values - jnp.mean(values, axis=1, keepdims=True)
    spread = jnp.mean(centred * centred, axis=1, keepdims=True)
    return (centred * lax.rsqrt(spread + EPS)).astype(jnp.bfloat16)


def gelu_pair(pre, d_act):
    act, pullback = jax.vjp(lambda v: jax.nn.gelu(v, approximate=True), pre)
    return (act.astype(jnp.bfloat16), pullback(d_act)[0].astype(jnp.bfloat16))


def outer_sum(left, right):
    return lax.dot_general(
        left, right, (((0,), (0,)), ((), ())), preferred_element_type=jnp.float32
    )


def regroup(snap_params, first_moment, second_moment, range_of_writer):
    flat = snap_params.shape[1]
    held = jnp.concatenate(
        [snap_params, first_moment.astype(jnp.bfloat16), second_moment.astype(jnp.bfloat16)],
        axis=1,
    )
    send = jnp.take(held, range_of_writer, axis=0).reshape(-1, 3, flat)
    got = lax.all_to_all(send, "group", split_axis=0, concat_axis=0, tiled=True)
    lines = jnp.swapaxes(got, 0, 1).reshape(3, 1, -1)
    return lines[0], lines[1:].astype(first_moment.dtype)


def matmul(left, right):
    return jnp.dot(left, right, preferred_element_type=jnp.float32)


def rounded_sum(left, right):
    total = left.astype(jnp.float32) + right.astype(jnp.float32)
    return total.astype(jnp.bfloat16)


def swap(values, step):
    pairs = [(i, i ^ step) for i in range(lax.axis_size("dp"))]
    return lax.ppermute(values, "dp", pairs)


def own_part(values, parts, part):
    rows = values.shape[0] // parts
    return lax.dynamic_slice_in_dim(values, part * rows, rows, axis=0)


def feature_columns(values):
    columns = values.shape[1] // 4
    me = lax.axis_index("dp")
    cut = [
        lax.dynamic_slice_in_dim(values, (me ^ r) * columns, columns, axis=1) for r in range(4)
    ]
    return [cut[0]] + [swap(cut[r], r) for r in (1, 2, 3)]


def sum_over_square(parts):
    half = parts[0].shape[0] // 2
    top, low = [p[:half] for p in parts], [p[half:] for p in parts]
    top_far, low_far = swap(top[3], 1), swap(low[3], 2)
    top_near, low_near = swap(top[1], 1), swap(low[2], 2)
    top_last = swap(rounded_sum(top[2], top_far), 2)
    low_last = swap(rounded_sum(low[1], low_far), 1)
    wide = jnp.float32
    return jnp.concatenate(
        [
            top[0].astype(wide) + top_near.astype(wide) + top_last.astype(wide),
            low[0].astype(wide) + low_near.astype(wide) + low_last.astype(wide),
        ],
        axis=0,
    )


def gather_over_square(block):
    half = block.shape[0] // 2
    first, second = swap(block, 1), swap(block, 2)
    across = jnp.concatenate([swap(first[:half], 2), swap(second[half:], 1)], axis=0)
    return first, second, across


def gradient(chunks, block):
    first, second, across = gather_over_square(block)
    near = outer_sum(
        jnp.concatenate(chunks[:3], axis=0), jnp.concatenate([block, first, second], axis=0)
    )
    return near + outer_sum(chunks[3], across)


def weight_gradients(tokens, frame_mask, cotangent, up_weight, down_weight):
    shares = lax.axis_size("group")
    group = lax.axis_index("group")
    mask = own_part(frame_mask, shares, group)[:, None].astype(jnp.bfloat16)
    masked = jnp.stack(feature_columns(own_part(cotangent, shares, group) * mask))
    masked = lax.all_gather(masked, "group", axis=0)
    masked = jnp.swapaxes(masked, 0, 1).reshape(4, tokens.shape[0], -1)
    masked = [masked[r] for r in range(4)]

    side = group % 2
    own = feature_columns(normalize(own_part(tokens, 2, side)))
    partner = [(i, i ^ 1) for i in range(shares)]
    normed = []
    for piece in own:
        other = lax.ppermute(piece, "group", partner)
        low = jnp.where(side == 0, piece, other)
        high = jnp.where(side == 0, other, piece)
        normed.append(jnp.concatenate([low, high], axis=0))

    pre = sum_over_square([matmul(n, up_weight).astype(jnp.bfloat16) for n in normed])
    d_act = sum_over_square([matmul(m, down_weight).astype(jnp.bfloat16) for m in masked])
    act, grad_pre = gelu_pair(pre, d_act)
    return gradient(normed, grad_pre), gradient(masked, act)


def weight_gradients_any(tokens, frame_mask, cotangent, up_weight, down_weight):
    shares = lax.axis_size("group")
    group = lax.axis_index("group")
    mask = own_part(frame_mask, shares, group)[:, None].astype(jnp.bfloat16)

    def to_features(rows_here):
        part = lax.all_to_all(rows_here, "dp", split_axis=1, concat_axis=0, tiled=True)
        return lax.all_gather(part, "group", axis=0, tiled=True)

    def own_rows_total(left, weight):
        part = matmul(left, weight).astype(jnp.bfloat16)
        return lax.psum_scatter(part, "dp", scatter_dimension=0, tiled=True).astype(jnp.float32)

    normed = to_features(normalize(own_part(tokens, shares, group)))
    masked = to_features(own_part(cotangent, shares, group) * mask)
    act, grad_pre = gelu_pair(
        own_rows_total(normed, up_weight), own_rows_total(masked, down_weight)
    )
    grad_down = outer_sum(masked, lax.all_gather(act, "dp", axis=0, tiled=True))
    grad_up = outer_sum(normed, lax.all_gather(grad_pre, "dp", axis=0, tiled=True))
    return grad_up, grad_down


def per_device(
    tokens,
    frame_mask,
    cotangent,
    up_weight,
    down_weight,
    snap_params,
    first_moment,
    second_moment,
    range_of_writer,
):
    written = regroup(snap_params, first_moment, second_moment, range_of_writer)
    square = lax.axis_size("dp") == 4 and lax.axis_size("group") % 2 == 0
    compute = weight_gradients if square else weight_gradients_any
    grads = compute(tokens, frame_mask, cotangent, up_weight, down_weight)
    return (*grads, *written)


def solution(mesh):
    placed = (
        P("dp", None),
        P("dp"),
        P("dp", None),
        P("dp", "group"),
        P("dp", "group"),
        P(None, ("dp", "group")),
        P(None, ("dp", "group")),
        P(None, ("dp", "group")),
        P(),
    )
    return jax.shard_map(
        per_device,
        mesh=mesh,
        in_specs=placed,
        out_specs=(P("dp", "group"), P("dp", "group"), P("group", "dp"), P(None, "group", "dp")),
        check_vma=False,
    )
```

```python
import jax
import jax.numpy as jnp
from jax import lax
from jax.sharding import PartitionSpec as P

EPS = 1e-06


def normalize(tokens):
    values = tokens.astype(jnp.float32)
    centred = values - jnp.mean(values, axis=1, keepdims=True)
    spread = jnp.mean(centred * centred, axis=1, keepdims=True)
    return (centred * lax.rsqrt(spread + EPS)).astype(jnp.bfloat16)


def gelu_pair(pre, d_act):
    act, pullback = jax.vjp(lambda v: jax.nn.gelu(v, approximate=True), pre)
    return (act.astype(jnp.bfloat16), pullback(d_act)[0].astype(jnp.bfloat16))


def outer_sum(left, right):
    return lax.dot_general(
        left, right, (((0,), (0,)), ((), ())), preferred_element_type=jnp.float32
    )


def regroup(snap_params, first_moment, second_moment, range_of_writer):
    flat = snap_params.shape[1]
    held = jnp.concatenate(
        [snap_params, first_moment.astype(jnp.bfloat16), second_moment.astype(jnp.bfloat16)],
        axis=1,
    )
    send = jnp.take(held, range_of_writer, axis=0).reshape(-1, 3, flat)
    got = lax.all_to_all(send, "group", split_axis=0, concat_axis=0, tiled=True)
    lines = jnp.swapaxes(got, 0, 1).reshape(3, 1, -1)
    return lines[0], lines[1:].astype(first_moment.dtype)


def matmul(left, right):
    return jnp.dot(left, right, preferred_element_type=jnp.float32)


def rounded_sum(left, right):
    total = left.astype(jnp.float32) + right.astype(jnp.float32)
    return total.astype(jnp.bfloat16)


def swap(values, step):
    pairs = [(i, i ^ step) for i in range(lax.axis_size("dp"))]
    return lax.ppermute(values, "dp", pairs)


def own_part(values, parts, part):
    rows = values.shape[0] // parts
    return lax.dynamic_slice_in_dim(values, part * rows, rows, axis=0)


def feature_columns(values):
    columns = values.shape[1] // 4
    me = lax.axis_index("dp")
    cut = [
        lax.dynamic_slice_in_dim(values, (me ^ r) * columns, columns, axis=1) for r in range(4)
    ]
    return [cut[0]] + [swap(cut[r], r) for r in (1, 2, 3)]


def sum_over_square(top, low):
    top_far, low_far = swap(top[3], 1), swap(low[3], 2)
    top_near, low_near = swap(top[1], 1), swap(low[2], 2)
    top_last = swap(rounded_sum(top[2], top_far), 2)
    low_last = swap(rounded_sum(low[1], low_far), 1)
    wide = jnp.float32
    return jnp.concatenate(
        [
            top[0].astype(wide) + top_near.astype(wide) + top_last.astype(wide),
            low[0].astype(wide) + low_near.astype(wide) + low_last.astype(wide),
        ],
        axis=0,
    )


def gather_over_square(block):
    half = block.shape[0] // 2
    first, second = swap(block, 1), swap(block, 2)
    across = jnp.concatenate([swap(first[:half], 2), swap(second[half:], 1)], axis=0)
    return first, second, across


def gradient(chunks, block):
    first, second, across = gather_over_square(block)
    near = outer_sum(
        jnp.concatenate(chunks[:3], axis=0), jnp.concatenate([block, first, second], axis=0)
    )
    near, across = lax.optimization_barrier((near, across))
    return near + outer_sum(chunks[3], across)


def weight_gradients(tokens, frame_mask, cotangent, up_weight, down_weight, written):
    shares = lax.axis_size("group")
    group = lax.axis_index("group")
    side = group % 2
    mask = own_part(frame_mask, shares, group)[:, None].astype(jnp.bfloat16)
    masked = own_part(cotangent, shares, group) * mask
    normed = normalize(own_part(tokens, 2, side))
    masked, normed = lax.optimization_barrier((masked, normed))

    masked = jnp.stack(feature_columns(masked))
    own = feature_columns(normed)
    partner = [(i, i ^ 1) for i in range(shares)]
    other = [lax.ppermute(piece, "group", partner) for piece in own]
    own[0], written = lax.optimization_barrier((own[0], written))

    masked = lax.all_gather(masked, "group", axis=0)
    lower, upper = masked[: shares // 2], masked[shares // 2 :]
    features = masked.shape[-1]

    def half(first, second):
        rows = jnp.swapaxes(jnp.where(side == 0, first, second), 0, 1)
        return list(rows.reshape(4, -1, features))

    ahead, behind = half(lower, upper), half(upper, lower)

    def partial(pieces, weight):
        return [matmul(piece, weight).astype(jnp.bfloat16) for piece in pieces]

    pre = sum_over_square(partial(own, up_weight), partial(other, up_weight))
    d_act = sum_over_square(partial(ahead, down_weight), partial(behind, down_weight))
    act, grad_pre = gelu_pair(pre, d_act)
    normed = [jnp.concatenate(pair, axis=0) for pair in zip(own, other)]
    masked = [jnp.concatenate(pair, axis=0) for pair in zip(ahead, behind)]
    return gradient(normed, grad_pre), gradient(masked, act), *written


def weight_gradients_any(tokens, frame_mask, cotangent, up_weight, down_weight, written):
    shares = lax.axis_size("group")
    group = lax.axis_index("group")
    mask = own_part(frame_mask, shares, group)[:, None].astype(jnp.bfloat16)

    def to_features(rows_here):
        part = lax.all_to_all(rows_here, "dp", split_axis=1, concat_axis=0, tiled=True)
        return lax.all_gather(part, "group", axis=0, tiled=True)

    def own_rows_total(left, weight):
        part = matmul(left, weight).astype(jnp.bfloat16)
        return lax.psum_scatter(part, "dp", scatter_dimension=0, tiled=True).astype(jnp.float32)

    normed = to_features(normalize(own_part(tokens, shares, group)))
    masked = to_features(own_part(cotangent, shares, group) * mask)
    act, grad_pre = gelu_pair(
        own_rows_total(normed, up_weight), own_rows_total(masked, down_weight)
    )
    grad_down = outer_sum(masked, lax.all_gather(act, "dp", axis=0, tiled=True))
    grad_up = outer_sum(normed, lax.all_gather(grad_pre, "dp", axis=0, tiled=True))
    return grad_up, grad_down, *written


def per_device(
    tokens,
    frame_mask,
    cotangent,
    up_weight,
    down_weight,
    snap_params,
    first_moment,
    second_moment,
    range_of_writer,
):
    written = regroup(snap_params, first_moment, second_moment, range_of_writer)
    square = lax.axis_size("dp") == 4 and lax.axis_size("group") % 2 == 0
    compute = weight_gradients if square else weight_gradients_any
    return compute(tokens, frame_mask, cotangent, up_weight, down_weight, written)


def solution(mesh):
    placed = (
        P("dp", None),
        P("dp"),
        P("dp", None),
        P("dp", "group"),
        P("dp", "group"),
        P(None, ("dp", "group")),
        P(None, ("dp", "group")),
        P(None, ("dp", "group")),
        P(),
    )
    return jax.shard_map(
        per_device,
        mesh=mesh,
        in_specs=placed,
        out_specs=(P("dp", "group"), P("dp", "group"), P("group", "dp"), P(None, "group", "dp")),
        check_vma=False,
    )
```

```python
import jax
import jax.numpy as jnp
from jax import lax
from jax.sharding import PartitionSpec as P

EPS = 1e-06


def normalize(tokens):
    values = tokens.astype(jnp.float32)
    centred = values - jnp.mean(values, axis=1, keepdims=True)
    spread = jnp.mean(centred * centred, axis=1, keepdims=True)
    return (centred * lax.rsqrt(spread + EPS)).astype(jnp.bfloat16)


def gelu_pair(pre, d_act):
    act, pullback = jax.vjp(lambda v: jax.nn.gelu(v, approximate=True), pre)
    return (act.astype(jnp.bfloat16), pullback(d_act)[0].astype(jnp.bfloat16))


def outer_sum(left, right):
    return lax.dot_general(
        left, right, (((0,), (0,)), ((), ())), preferred_element_type=jnp.float32
    )


def regroup(snap_params, first_moment, second_moment, range_of_writer):
    flat = snap_params.shape[1]
    held = jnp.concatenate(
        [snap_params, first_moment.astype(jnp.bfloat16), second_moment.astype(jnp.bfloat16)],
        axis=1,
    )
    send = jnp.take(held, range_of_writer, axis=0).reshape(-1, 3, flat)
    got = lax.all_to_all(send, "group", split_axis=0, concat_axis=0, tiled=True)
    lines = jnp.swapaxes(got, 0, 1).reshape(3, 1, -1)
    return lines[0], lines[1:].astype(first_moment.dtype)


def matmul(left, right):
    return jnp.dot(left, right, preferred_element_type=jnp.float32)


def rounded_sum(left, right):
    total = left.astype(jnp.float32) + right.astype(jnp.float32)
    return total.astype(jnp.bfloat16)


def swap(values, step):
    pairs = [(i, i ^ step) for i in range(lax.axis_size("dp"))]
    return lax.ppermute(values, "dp", pairs)


def own_part(values, parts, part):
    rows = values.shape[0] // parts
    return lax.dynamic_slice_in_dim(values, part * rows, rows, axis=0)


def feature_columns(values):
    columns = values.shape[1] // 4
    me = lax.axis_index("dp")
    cut = [
        lax.dynamic_slice_in_dim(values, (me ^ r) * columns, columns, axis=1) for r in range(4)
    ]
    return [cut[0]] + [swap(cut[r], r) for r in (1, 2, 3)]


def sum_over_square(parts):
    half = parts[0].shape[0] // 2
    top, low = [p[:half] for p in parts], [p[half:] for p in parts]
    top_far, low_far = swap(top[3], 1), swap(low[3], 2)
    top_near, low_near = swap(top[1], 1), swap(low[2], 2)
    top_last = swap(rounded_sum(top[2], top_far), 2)
    low_last = swap(rounded_sum(low[1], low_far), 1)
    wide = jnp.float32
    return jnp.concatenate(
        [
            top[0].astype(wide) + top_near.astype(wide) + top_last.astype(wide),
            low[0].astype(wide) + low_near.astype(wide) + low_last.astype(wide),
        ],
        axis=0,
    )


def gather_over_square(block):
    half = block.shape[0] // 2
    first, second = swap(block, 1), swap(block, 2)
    across = jnp.concatenate([swap(first[:half], 2), swap(second[half:], 1)], axis=0)
    return first, second, across


def gradient(chunks, block):
    first, second, across = gather_over_square(block)
    near = outer_sum(
        jnp.concatenate(chunks[:3], axis=0), jnp.concatenate([block, first, second], axis=0)
    )
    near, across = lax.optimization_barrier((near, across))
    return near + outer_sum(chunks[3], across)


def weight_gradients(tokens, frame_mask, cotangent, up_weight, down_weight, *snapshot):
    shares = lax.axis_size("group")
    group = lax.axis_index("group")
    mask = own_part(frame_mask, shares, group)[:, None].astype(jnp.bfloat16)
    masked = jnp.stack(feature_columns(own_part(cotangent, shares, group) * mask))
    masked = lax.all_gather(masked, "group", axis=0)
    masked = jnp.swapaxes(masked, 0, 1).reshape(4, tokens.shape[0], -1)
    masked = [masked[r] for r in range(4)]

    side = group % 2
    own = feature_columns(normalize(own_part(tokens, 2, side)))
    own[0], snapshot = lax.optimization_barrier((own[0], snapshot))
    written = regroup(*snapshot)
    partner = [(i, i ^ 1) for i in range(shares)]
    normed = []
    for piece in own:
        other = lax.ppermute(piece, "group", partner)
        low = jnp.where(side == 0, piece, other)
        high = jnp.where(side == 0, other, piece)
        normed.append(jnp.concatenate([low, high], axis=0))

    normed[0], written = lax.optimization_barrier((normed[0], written))
    pre = sum_over_square([matmul(n, up_weight).astype(jnp.bfloat16) for n in normed])
    d_act = sum_over_square([matmul(m, down_weight).astype(jnp.bfloat16) for m in masked])
    act, grad_pre = gelu_pair(pre, d_act)
    return gradient(normed, grad_pre), gradient(masked, act), *written


def weight_gradients_any(tokens, frame_mask, cotangent, up_weight, down_weight, *snapshot):
    shares = lax.axis_size("group")
    group = lax.axis_index("group")
    mask = own_part(frame_mask, shares, group)[:, None].astype(jnp.bfloat16)

    def to_features(rows_here):
        part = lax.all_to_all(rows_here, "dp", split_axis=1, concat_axis=0, tiled=True)
        return lax.all_gather(part, "group", axis=0, tiled=True)

    def own_rows_total(left, weight):
        part = matmul(left, weight).astype(jnp.bfloat16)
        return lax.psum_scatter(part, "dp", scatter_dimension=0, tiled=True).astype(jnp.float32)

    normed = to_features(normalize(own_part(tokens, shares, group)))
    masked = to_features(own_part(cotangent, shares, group) * mask)
    act, grad_pre = gelu_pair(
        own_rows_total(normed, up_weight), own_rows_total(masked, down_weight)
    )
    grad_down = outer_sum(masked, lax.all_gather(act, "dp", axis=0, tiled=True))
    grad_up = outer_sum(normed, lax.all_gather(grad_pre, "dp", axis=0, tiled=True))
    return grad_up, grad_down, *regroup(*snapshot)


def per_device(
    tokens,
    frame_mask,
    cotangent,
    up_weight,
    down_weight,
    snap_params,
    first_moment,
    second_moment,
    range_of_writer,
):
    square = lax.axis_size("dp") == 4 and lax.axis_size("group") % 2 == 0
    compute = weight_gradients if square else weight_gradients_any
    snapshot = (snap_params, first_moment, second_moment, range_of_writer)
    return compute(tokens, frame_mask, cotangent, up_weight, down_weight, *snapshot)


def solution(mesh):
    placed = (
        P("dp", None),
        P("dp"),
        P("dp", None),
        P("dp", "group"),
        P("dp", "group"),
        P(None, ("dp", "group")),
        P(None, ("dp", "group")),
        P(None, ("dp", "group")),
        P(),
    )
    return jax.shard_map(
        per_device,
        mesh=mesh,
        in_specs=placed,
        out_specs=(P("dp", "group"), P("dp", "group"), P("group", "dp"), P(None, "group", "dp")),
        check_vma=False,
    )
```
